32 devices in a mesh: groups: 2 (over y), tensor: 4 (over z), dp: 2 (over x), kv: 2 (over core).
Axes of the slice: x: 2, y: 2, z: 4, core: 2. Of those that a mesh axis runs over, the one named last changes fastest.
Arguments:
- residual: bfloat16 [64, 16384], P(('groups', 'dp'), ('tensor', 'kv')), parts along dimension 0, may hold values from -10 to 10
- query: bfloat16 [64, 8192], P(('groups', 'dp'), ('tensor', 'kv')), parts along dimension 0, may hold values from -60 to 60
- new_pair: bfloat16 [2, 64, 4, 128], P(None, ('groups', 'dp')), parts along dimension 1, may hold values from -8 to 8
- kv_cache: bfloat16 [2, 64, 2048, 4, 128], P(None, ('groups', 'dp'), ('tensor', 'kv')), parts along dimension 1, may hold values from -4.5 to 4.5
- lengths: int32 [64], P(('groups', 'dp')), parts along dimension 0, may hold values from 2 to 2048
- out_weight: bfloat16 [8192, 16384], P(('tensor', 'kv')), may hold values from -0.09375 to 0.09375
- norm_gain: bfloat16 [16384], replicated, may hold values from 0.25 to 1.75
Outputs:
- residual_out: bfloat16 [64, 16384], P(('groups', 'dp'), ('tensor', 'kv')), parts along dimension 0
- mlp_input: bfloat16 [64, 16384], P(('groups', 'dp')), parts along dimension 0
The draws below stay inside these ranges and needn't reach their ends.
There are 2 independent parts, one for each index of `groups`. The reference program is written for one: setup_inputs(seed, part) draws one part's arguments, and reference() takes and returns one part's arrays. A program takes and returns all parts, laid end to end along the dimension named above; an argument that names none is the same for every part. Nothing has to cross between parts.
Inputs may be any that keep to these rules, and one draw needn't show every extreme that they name: Positions below lengths[b] hold sequence b's cache; the others are ignored.
All inputs are finite; a program needn't handle non-finite values.
Results may differ from the reference program's by a relative error of at most 0.007.
Values may be sent and summed in bfloat16 or wider, within the bound.
A program may use at most 128 MiB of HBM per device.

```python
import math
import jax
import jax.numpy as jnp
from jax import lax

D = 16384
QH = 64
KVH = 4
HD = 128
MAXLEN = 2048
B = 32


def cache_values(key):
    shape = (2, B, MAXLEN, KVH, HD)
    base = jnp.clip(jax.random.normal(jax.random.fold_in(key, 101), shape, jnp.float32), -4.5, 4.5)
    return base


def draw_kv_cache(key, part):
    return cache_values(key).astype(jnp.bfloat16)


def draw_query(key, part):
    drawn = jnp.clip(1.5 * jax.random.normal(jax.random.fold_in(key, 202), (B, QH, HD), jnp.float32), -9.0, 9.0)
    return drawn.reshape(B, QH * HD).astype(jnp.bfloat16)


def draw_residual(key, part):
    noise_key = jax.random.fold_in(key, 303)
    column_key = jax.random.fold_in(key, 304)
    row_key = jax.random.fold_in(key, 305)
    columns = jnp.arange(D, dtype=jnp.float32) / D
    column_scale = jnp.exp(jax.random.uniform(column_key, (D,), jnp.float32, 0.0, math.log(10.0)))
    row_scale = jnp.exp(jax.random.uniform(row_key, (B, 1), jnp.float32, 0.0, math.log(10.0)))
    raw = jnp.clip(jax.random.normal(noise_key, (B, D), jnp.float32), -6.0, 6.0)
    rising = jnp.power(3.0, columns)
    base = 0.005
    return (base * raw * rising[None, :] * column_scale[None, :] * row_scale).astype(jnp.bfloat16)


def set_ends(drawn, rng, low, largest):
    longest = drawn.shape.index(max(drawn.shape))
    spots = []
    for shift in (0, 1):
        where = [jax.random.randint(jax.random.fold_in(rng, axis), (), 0, length) for axis, length in enumerate(drawn.shape)]
        where[longest] = (where[longest] + shift) % drawn.shape[longest]
        spots.append(tuple(where))
    return drawn.at[spots[0]].set(low).at[spots[1]].set(largest)


def spiked(array, stream_key, source, target, shards_of, factor):
    def block_of(dim):
        return (jnp.arange(array.shape[dim]) // (array.shape[dim] // shards_of)).reshape((-1,) + (1,) * (array.ndim - 1 - dim))

    one_side = jax.random.permutation(stream_key, shards_of)[block_of(target)]
    other_side = (block_of(target) + shards_of // 2) % shards_of
    return jnp.where((block_of(source) == one_side) | (block_of(source) == other_side), factor * array, array)


def levels(rng, shape, split, smallest, top_value):
    gain, own = 1.0, jax.random.fold_in(rng, 6)
    for dim, parts in split:
        steps = jnp.exp(jax.random.uniform(jax.random.fold_in(own, dim), (parts,), jnp.float32, smallest / len(split), top_value / len(split)))
        gain = gain * jnp.repeat(steps, shape[dim] // parts).reshape([-1 if axis == dim else 1 for axis in range(len(shape))])
    return gain


def bell_draw(rng, dims, spread, limit, shards=(), kind=jnp.bfloat16):
    array = spread * jax.random.normal(rng, dims, jnp.float32)
    if shards:
        array = array * levels(rng, dims, shards, -0.22, 0.18)
    return jnp.clip(array, -limit, limit).astype(kind)


def noise_with(key, shape, deviation, most, cuts, heavy, kind=jnp.bfloat16):
    drawn = deviation * jax.random.normal(key, shape, jnp.float32)
    if cuts:
        drawn = drawn * levels(key, shape, cuts, -0.22, 0.18)
    return jnp.clip(spiked(drawn, jax.random.fold_in(key, 3), *heavy), -most, most).astype(kind)


def setup_inputs(seed: int = 0, part: int = 0) -> dict:
    splits = jax.random.split(jax.random.key(seed), 8)
    part_splits = jax.random.split(jax.random.fold_in(splits[7], part), 8)
    return {
        "residual": draw_residual(jax.random.fold_in(jax.random.fold_in(splits[7], part), 71), part),
        "query": draw_query(jax.random.fold_in(jax.random.fold_in(splits[7], part), 71), part),
        "new_pair": bell_draw(part_splits[2], (2, B, KVH, HD), 1.5, 8.0, ((1, 2),)),
        "kv_cache": draw_kv_cache(jax.random.fold_in(jax.random.fold_in(splits[7], part), 71), part),
        "lengths": set_ends(jax.random.randint(part_splits[4], (B,), 2, MAXLEN + 1), jax.random.fold_in(part_splits[4], 1), 2, MAXLEN).astype(jnp.int32),
        "out_weight": noise_with(splits[5], (QH * HD, D), (QH * HD) ** -0.5, 0.09375, ((0, 8),), (0, 1, 8, 2.0)),
        "norm_gain": jnp.clip(1.0 + 0.15 * jax.random.normal(splits[6], (D,), jnp.float32), 0.25, 1.75).astype(jnp.bfloat16),
    }


floor_value = -1e+30
epsilon = 1e-05

def reference(residual, query, new_pair, kv_cache, lengths, out_weight, norm_gain):
    batch = residual.shape[0]
    group = QH // KVH
    scaling = 1.0 / math.sqrt(HD)
    grouped = query.astype(jnp.float32).reshape(batch, KVH, group, HD)
    keys = kv_cache[0].astype(jnp.float32)
    values = kv_cache[1].astype(jnp.float32)
    scores = jnp.einsum('bgjd,bpgd->bgjp', grouped, keys, precision=lax.Precision.HIGHEST) * scaling
    places = jnp.arange(MAXLEN, dtype=jnp.int32)
    live = (places[None, :] < lengths[:, None])[:, None, None, :]
    scores = jnp.where(live, scores, floor_value)
    fresh_key = new_pair[0].astype(jnp.float32)
    fresh_value = new_pair[1].astype(jnp.float32)
    fresh = jnp.einsum('bgjd,bgd->bgj', grouped, fresh_key, precision=lax.Precision.HIGHEST) * scaling
    highest = jnp.maximum(lax.optimization_barrier(jnp.max(scores, axis=3)), fresh)
    weights = jnp.where(live, jnp.exp(scores - highest[..., None]), 0.0)
    fresh_weight = jnp.exp(fresh - highest)
    totals = lax.optimization_barrier(jnp.sum(weights, axis=3)) + fresh_weight
    accum = jnp.einsum('bgjp,bpgd->bgjd', weights, values, precision=lax.Precision.HIGHEST)
    accum = accum + fresh_weight[..., None] * fresh_value[:, :, None, :]
    attended = (accum / totals[..., None]).astype(jnp.bfloat16).reshape(batch, QH * HD)
    projected = jnp.dot(attended, out_weight, preferred_element_type=jnp.float32)
    stream = (residual.astype(jnp.float32) + projected).astype(jnp.bfloat16)
    widened = stream.astype(jnp.float32)
    mean_square = lax.optimization_barrier(jnp.mean(widened * widened, axis=1))
    normed = widened * lax.rsqrt(mean_square + epsilon)[:, None] * norm_gain.astype(jnp.float32)[None, :]
    return (stream, normed.astype(jnp.bfloat16))
```

```python
import functools
import math

import jax
import jax.numpy as jnp
from jax import lax
from jax.experimental import pallas as pl
from jax.experimental.pallas import tpu as pltpu
from jax.sharding import PartitionSpec as P

HD = 128
LANES = 128
floor_value = -1e30
epsilon = 1e-05
MESH = pl.DeviceIdType.MESH


def kernel(
    T, K, kvh,
    lens_ref, q_ref, pair_ref, kv_hbm, w_hbm, res_ref, gain_ref,
    stream_ref, out_ref,
    kv, wbuf, qg, qf, of, lf, colid, abuf, arecv, fpart, pbuf, precv, zbuf, zrecv, full, lhs,
    kv_sem, w_sem, qs, qr, qfs, qfr, asend, ars, ps, pr, zs, zr, gs, gr, gfs, gfr,
):
    t = lax.axis_index("tensor")
    k = lax.axis_index("kv")
    n = T * K
    mine = t * K + k
    other = K - 1 - k
    S, width = res_ref.shape
    ph = q_ref.shape[1] // HD
    QH = ph * n
    group = QH // kvh
    C = kv.shape[2]
    span = C // kvh
    D = out_ref.shape[1]

    def kv_copy(i, b):
        return pltpu.make_async_copy(kv_hbm.at[i, b], kv.at[i, b], kv_sem.at[i, b])

    @pl.loop(0, S)
    def _(b):
        kv_copy(0, b).start()
        kv_copy(1, b).start()

    def hop(s):
        return lax.rem(t + 1 + s, T)

    def origin(s):
        return lax.rem(t + T - 1 - s, T)

    def w_copy(s):
        if s < T:
            dest = hop(s) * K + other
        else:
            dest = hop(s - T) * K + k
        cols = pl.ds(pl.multiple_of(dest * width, width), width)
        return pltpu.make_async_copy(w_hbm.at[:, cols], wbuf.at[s], w_sem.at[s])

    for s in range(n):
        w_copy(s).start()

    barrier = pltpu.get_barrier_semaphore()
    for p in range(1, n):
        j = lax.rem(mine + p, n)
        pl.semaphore_signal(
            barrier, inc=1, device_id={"tensor": j // K, "kv": lax.rem(j, K)}, device_id_type=MESH
        )
    qg[mine] = q_ref[...]
    pl.semaphore_wait(barrier, n - 1)

    def remote(src, dst, ss, rs, tt, kk):
        return pltpu.make_async_remote_copy(
            src_ref=src, dst_ref=dst, send_sem=ss, recv_sem=rs,
            device_id={"tensor": tt, "kv": kk}, device_id_type=MESH,
        )

    def gather_start(buf, ss, rs):
        out = []
        for s in range(T - 1):
            c = remote(buf.at[mine], buf.at[mine], ss.at[s], rs.at[s], hop(s), k)
            c.start()
            out.append(c)
        c = remote(buf.at[mine], buf.at[mine], ss.at[T - 1], rs.at[T - 1], t, other)
        c.start()
        out.append(c)
        return out

    def gather_finish(buf, copies, fs, fr):
        fwd = []
        order = sorted(range(T - 1), key=lambda s: min(s + 1, T - 1 - s))
        for s in order:
            copies[s].wait_recv()
            j = origin(s) * K + k
            c = remote(buf.at[j], buf.at[j], fs.at[s], fr.at[s], t, other)
            c.start()
            fwd.append(c)
        copies[T - 1].wait_recv()
        for c in fwd:
            c.wait_recv()
        return fwd

    qcopies = gather_start(qg, qs, qr)

    col = lax.broadcasted_iota(jnp.int32, (QH, C), 1)
    head = lax.broadcasted_iota(jnp.int32, (QH, C), 0)
    colid[...] = jnp.where(lax.rem(col, kvh) == head // group, col, jnp.int32(2**30))
    scale2 = math.log2(math.e) / math.sqrt(HD)
    my_group = (mine * ph) // group
    fkey = jnp.zeros((S, HD), jnp.float32)
    fval = jnp.zeros((S, HD), jnp.float32)
    for g in range(kvh):
        lanes = slice(g * HD, (g + 1) * HD)
        fkey = jnp.where(my_group == g, pair_ref[0, :, lanes].astype(jnp.float32), fkey)
        fval = jnp.where(my_group == g, pair_ref[1, :, lanes].astype(jnp.float32), fval)
    lane = lax.broadcasted_iota(jnp.int32, (S, LANES), 1)
    fresh = jnp.zeros((S, LANES), jnp.float32)
    for h in range(ph):
        prod = q_ref[:, h * HD:(h + 1) * HD].astype(jnp.float32) * fkey
        fresh = jnp.where(lane == h, jnp.sum(prod, axis=1, keepdims=True) * scale2, fresh)
    fpart[0] = fresh
    fpart[1] = fval

    qfwd = gather_finish(qg, qcopies, qfs, qfr)
    for j in range(n):
        for h in range(ph):
            r = (j * ph + h) * S
            qf[r:r + S, :] = qg[j, :, h * HD:(h + 1) * HD].astype(jnp.float32)

    start = mine * span

    def attend(b, _):
        kv_copy(0, b).wait()
        kv_copy(1, b).wait()
        qb = qf[pl.ds(b, QH, stride=S), :].astype(jnp.bfloat16)
        s = lax.dot_general(qb, kv[0, b], (((1,), (1,)), ((), ())), preferred_element_type=jnp.float32)
        lim = (lens_ref[b] - start) * kvh
        s = jnp.where(colid[...] < lim, s * scale2, floor_value)
        m = jnp.maximum(jnp.max(s, axis=1, keepdims=True), -1e29)
        p = jnp.exp2(s - m)
        l = jnp.maximum(jnp.sum(p, axis=1, keepdims=True), 1.0)
        o = jnp.dot(p.astype(jnp.bfloat16), kv[1, b], preferred_element_type=jnp.float32)
        of[pl.ds(b, QH, stride=S), :] = o / l
        lf[pl.ds(b, QH, stride=S), :] = jnp.broadcast_to(m + jnp.log2(l), (QH, LANES))
        return 0

    lax.fori_loop(0, S, attend, 0)

    low = lax.rem(lane, 32)
    for j in range(n):
        tot = jnp.zeros((S, LANES), jnp.float32)
        for h in range(ph):
            r = (j * ph + h) * S
            abuf[j, :, h * HD:(h + 1) * HD] = of[r:r + S, :].astype(jnp.bfloat16)
            tot = jnp.where(low == h, lf[r:r + S, :], tot)
        hi = tot.astype(jnp.bfloat16).astype(jnp.float32)
        mid = (tot - hi).astype(jnp.bfloat16).astype(jnp.float32)
        rest = tot - hi - mid
        packed = jnp.where(lane < 32, hi, jnp.where(lane < 64, mid, rest))
        abuf[j, :, ph * HD:] = packed.astype(jnp.bfloat16)
    acopies = []
    for p in range(1, n):
        j = lax.rem(mine + p, n)
        c = remote(abuf.at[j], arecv.at[mine], asend.at[p], ars.at[p], j // K, lax.rem(j, K))
        c.start()
        acopies.append(c)
    arecv[mine] = abuf[mine]
    for c in acopies:
        c.wait_recv()

    fresh = fpart[0]
    lse = []
    best = fresh
    for j in range(n):
        e = arecv[j, :, ph * HD:].astype(jnp.float32)
        e = e + pltpu.roll(e, 96, 1) + pltpu.roll(e, 64, 1)
        lse.append(e)
        best = jnp.maximum(best, e)
    fw = jnp.exp2(fresh - best)
    total = fw
    ws = []
    for j in range(n):
        w = jnp.exp2(lse[j] - best)
        ws.append(w)
        total = total + w
    inv = 1.0 / total
    for h in range(ph):
        acc = (fw * inv)[:, h:h + 1] * fpart[1]
        for j in range(n):
            acc = acc + (ws[j] * inv)[:, h:h + 1] * arecv[j, :, h * HD:(h + 1) * HD].astype(jnp.float32)
        lhs[:, h * HD:(h + 1) * HD] = acc.astype(jnp.bfloat16)

    tile = min(width, 512)

    pcopies = []
    for s in range(T):
        w_copy(s).wait()

        @pl.loop(0, width // tile)
        def _(i):
            cols = pl.ds(pl.multiple_of(i * tile, tile), tile)
            y = jnp.dot(lhs[...], wbuf[s, :, cols], preferred_element_type=jnp.float32)
            pbuf[s, :, cols] = y.astype(jnp.bfloat16)

        c = remote(pbuf.at[s], precv.at[s], ps.at[s], pr.at[s], t, other)
        c.start()
        pcopies.append(c)
    zcopies = []
    for s in range(T):
        w_copy(T + s).wait()
        pcopies[s].wait_recv()

        @pl.loop(0, width // tile)
        def _(i):
            cols = pl.ds(pl.multiple_of(i * tile, tile), tile)
            y = jnp.dot(lhs[...], wbuf[T + s, :, cols], preferred_element_type=jnp.float32)
            y = y + precv[s, :, cols].astype(jnp.float32)
            if s < T - 1:
                zbuf[s, :, cols] = y.astype(jnp.bfloat16)
            else:
                out = y + res_ref[:, cols].astype(jnp.float32)
                for u in range(tile // LANES):
                    qf[pl.ds(pl.multiple_of((i * (tile // LANES) + u) * S, S), S), :] = (
                        out[:, u * LANES:(u + 1) * LANES]
                    )

        if s < T - 1:
            c = remote(zbuf.at[s], zrecv.at[s], zs.at[s], zr.at[s], hop(s), k)
            c.start()
            zcopies.append(c)
    for c in zcopies:
        c.wait_recv()
    for u in range(width // LANES):
        cols = slice(u * LANES, (u + 1) * LANES)
        x = qf[u * S:(u + 1) * S, :]
        for s in range(T - 1):
            x = x + zrecv[s, :, cols].astype(jnp.float32)
        x = x.astype(jnp.bfloat16)
        full[mine, :, cols] = x
        stream_ref[:, cols] = x

    gcopies = gather_start(full, gs, gr)
    gfwd = gather_finish(full, gcopies, gfs, gfr)

    sq = jnp.zeros((S, width), jnp.float32)
    for j in range(n):
        x = full[j].astype(jnp.float32)
        sq = sq + x * x
    r = lax.rsqrt(jnp.sum(sq, axis=1, keepdims=True) / D + epsilon)
    for j in range(n):
        cols = slice(j * width, (j + 1) * width)
        x = full[j].astype(jnp.float32) * r * gain_ref[:, cols].astype(jnp.float32)
        out_ref[:, cols] = x.astype(jnp.bfloat16)

    for c in qcopies + qfwd + acopies + pcopies + zcopies + gcopies + gfwd:
        c.wait_send()


def on_device(T, K, residual, query, new_pair, kv_cache, lengths, out_weight, norm_gain):
    n = T * K
    S, width = residual.shape
    ph = query.shape[1] // HD
    span, kvh = kv_cache.shape[2:4]
    C = span * kvh
    QH = ph * n
    D = out_weight.shape[1]
    vm = pl.BlockSpec(memory_space=pltpu.VMEM)
    hbm = pl.BlockSpec(memory_space=pl.ANY)
    bf = jnp.bfloat16
    dma = pltpu.SemaphoreType.DMA
    scratch = [
        pltpu.VMEM((2, S, C, HD), bf),
        pltpu.VMEM((n, ph * HD, width), bf),
        pltpu.VMEM((n, S, ph * HD), bf),
        pltpu.VMEM((QH * S, HD), jnp.float32),
        pltpu.VMEM((QH * S, HD), jnp.float32),
        pltpu.VMEM((QH * S, LANES), jnp.float32),
        pltpu.VMEM((QH, C), jnp.int32),
        pltpu.VMEM((n, S, (ph + 1) * HD), bf),
        pltpu.VMEM((n, S, (ph + 1) * HD), bf),
        pltpu.VMEM((2, S, LANES), jnp.float32),
        pltpu.VMEM((T, S, width), bf),
        pltpu.VMEM((T, S, width), bf),
        pltpu.VMEM((T, S, width), bf),
        pltpu.VMEM((T, S, width), bf),
        pltpu.VMEM((n, S, width), bf),
        pltpu.VMEM((S, ph * HD), bf),
        dma((2, S)),
        dma((n,)),
        dma((T,)), dma((T,)), dma((T,)), dma((T,)),
        dma((n,)), dma((n,)),
        dma((T,)), dma((T,)),
        dma((T,)), dma((T,)),
        dma((T,)), dma((T,)), dma((T,)), dma((T,)),
    ]
    return pl.pallas_call(
        functools.partial(kernel, T, K, kvh),
        out_shape=(
            jax.ShapeDtypeStruct((S, width), bf),
            jax.ShapeDtypeStruct((S, D), bf),
        ),
        in_specs=[pl.BlockSpec(memory_space=pltpu.SMEM), vm, vm, hbm, hbm, vm, vm],
        out_specs=(vm, vm),
        scratch_shapes=scratch,
        compiler_params=pltpu.CompilerParams(
            collective_id=0, has_side_effects=True, vmem_limit_bytes=60 * 1024 * 1024
        ),
    )(
        lengths,
        query,
        new_pair.reshape(2, S, kvh * HD),
        kv_cache.reshape(2, S, C, HD),
        out_weight,
        residual,
        norm_gain.reshape(1, D),
    )


def solution(mesh):
    T, K = mesh.shape["tensor"], mesh.shape["kv"]
    seqs = ("groups", "dp")
    split = ("tensor", "kv")
    placed = (
        P(seqs, split),
        P(seqs, split),
        P(None, seqs, None, None),
        P(None, seqs, split, None, None),
        P(seqs),
        P(split, None),
        P(),
    )
    return jax.shard_map(
        functools.partial(on_device, T, K),
        mesh=mesh,
        in_specs=placed,
        out_specs=(P(seqs, split), P(seqs, None)),
        check_vma=False,
    )
```

```python
import functools
import math

import jax
import jax.numpy as jnp
from jax import lax
from jax.experimental import pallas as pl
from jax.experimental.pallas import tpu as pltpu
from jax.sharding import PartitionSpec as P

HD = 128
LANES = 128
floor_value = -1e30
epsilon = 1e-05
MESH = pl.DeviceIdType.MESH
VOUT = pltpu.VMEM


def kernel(
    T, K, kvh,
    lens_ref, q_hbm, pair_hbm, kv_hbm, w_hbm, res_hbm,
    stream_ref, full,
    pair_ref, res_ref, ybuf, kv, wbuf, qg, qf, of, lf, colid, abuf, arecv, fpart, pbuf, precv, zbuf, zrecv, lhs,
    small_sem, kv_sem, w_sem, qs, qr, qfs, qfr, asend, ars, ps, pr, zs, zr, gs, gr, gfs, gfr,
):
    t = lax.axis_index("tensor")
    k = lax.axis_index("kv")
    n = T * K
    mine = t * K + k
    other = K - 1 - k
    S, width = res_ref.shape
    ph = q_hbm.shape[1] // HD
    QH = ph * n
    group = QH // kvh
    C = kv.shape[2]
    span = C // kvh
    rows = S // 2

    barrier = pltpu.get_barrier_semaphore()
    for p in range(1, n):
        j = lax.rem(mine + p, n)
        pl.semaphore_signal(
            barrier, inc=1, device_id={"tensor": j // K, "kv": lax.rem(j, K)}, device_id_type=MESH
        )

    small = [
        pltpu.make_async_copy(q_hbm, qg.at[mine], small_sem.at[0]),
        pltpu.make_async_copy(pair_hbm, pair_ref, small_sem.at[1]),
        pltpu.make_async_copy(res_hbm, res_ref, small_sem.at[2]),
    ]
    for c in small:
        c.start()

    def kv_copy(i, b):
        return pltpu.make_async_copy(kv_hbm.at[i, b], kv.at[i, b], kv_sem.at[i, b])

    @pl.loop(0, S)
    def _(b):
        kv_copy(0, b).start()
        kv_copy(1, b).start()

    def hop(s):
        return lax.rem(t + 1 + s, T)

    def origin(s):
        return lax.rem(t + T - 1 - s, T)

    def w_copy(s):
        dest = hop(s // 2) * K + (k if s % 2 else other)
        cols = pl.ds(pl.multiple_of(dest * width, width), width)
        return pltpu.make_async_copy(w_hbm.at[:, cols], wbuf.at[s], w_sem.at[s])

    for s in range(n):
        w_copy(s).start()

    small[0].wait()
    pl.semaphore_wait(barrier, n - 1)

    def remote(src, dst, ss, rs, tt, kk):
        return pltpu.make_async_remote_copy(
            src_ref=src, dst_ref=dst, send_sem=ss, recv_sem=rs,
            device_id={"tensor": tt, "kv": kk}, device_id_type=MESH,
        )

    def gather_start(buf, ss, rs):
        out = []
        for s in range(T - 1):
            c = remote(buf.at[mine], buf.at[mine], ss.at[s], rs.at[s], hop(s), k)
            c.start()
            out.append(c)
        c = remote(buf.at[mine], buf.at[mine], ss.at[T - 1], rs.at[T - 1], t, other)
        c.start()
        out.append(c)
        return out

    def gather_finish(buf, copies, fs, fr):
        fwd = []
        order = sorted(range(T - 1), key=lambda s: min(s + 1, T - 1 - s))
        for s in order:
            copies[s].wait_recv()
            j = origin(s) * K + k
            c = remote(buf.at[j], buf.at[j], fs.at[s], fr.at[s], t, other)
            c.start()
            fwd.append(c)
        copies[T - 1].wait_recv()
        for c in fwd:
            c.wait_recv()
        return fwd

    qcopies = gather_start(qg, qs, qr)

    col = lax.broadcasted_iota(jnp.int32, (QH, C), 1)
    head = lax.broadcasted_iota(jnp.int32, (QH, C), 0)
    colid[...] = jnp.where(lax.rem(col, kvh) == head // group, col, jnp.int32(2**30))
    scale2 = math.log2(math.e) / math.sqrt(HD)
    my_group = (mine * ph) // group
    fkey = jnp.zeros((S, HD), jnp.float32)
    fval = jnp.zeros((S, HD), jnp.float32)
    small[1].wait()
    small[2].wait()
    for g in range(kvh):
        fkey = jnp.where(my_group == g, pair_ref[0, :, g, :].astype(jnp.float32), fkey)
        fval = jnp.where(my_group == g, pair_ref[1, :, g, :].astype(jnp.float32), fval)
    lane = lax.broadcasted_iota(jnp.int32, (S, LANES), 1)
    fresh = jnp.zeros((S, LANES), jnp.float32)
    for h in range(ph):
        prod = qg[mine, :, h * HD:(h + 1) * HD].astype(jnp.float32) * fkey
        fresh = jnp.where(lane == h, jnp.sum(prod, axis=1, keepdims=True) * scale2, fresh)
    fpart[0] = fresh
    fpart[1] = fval

    qfwd = gather_finish(qg, qcopies, qfs, qfr)
    for j in range(n):
        for h in range(ph):
            r = (j * ph + h) * S
            qf[r:r + S, :] = qg[j, :, h * HD:(h + 1) * HD].astype(jnp.float32)

    start = mine * span

    def attend(b, _):
        kv_copy(0, b).wait()
        kv_copy(1, b).wait()
        qb = qf[pl.ds(b, QH, stride=S), :].astype(jnp.bfloat16)
        s = lax.dot_general(qb, kv[0, b], (((1,), (1,)), ((), ())), preferred_element_type=jnp.float32)
        lim = (lens_ref[b] - start) * kvh
        s = jnp.where(colid[...] < lim, s * scale2, floor_value)
        m = jnp.maximum(jnp.max(s, axis=1, keepdims=True), -1e29)
        p = jnp.exp2(s - m)
        l = jnp.maximum(jnp.sum(p, axis=1, keepdims=True), 1.0)
        o = jnp.dot(p.astype(jnp.bfloat16), kv[1, b], preferred_element_type=jnp.float32)
        of[pl.ds(b, QH, stride=S), :] = o / l
        lf[pl.ds(b, QH, stride=S), :] = jnp.broadcast_to(m + jnp.log2(l), (QH, LANES))
        return 0

    lane = lax.broadcasted_iota(jnp.int32, (rows, LANES), 1)
    low = lax.rem(lane, 32)
    acopies = []
    for half in range(2):
        lax.fori_loop(half * rows, (half + 1) * rows, attend, 0, unroll=4)
        for j in range(n):
            tot = jnp.zeros((rows, LANES), jnp.float32)
            for h in range(ph):
                r = (j * ph + h) * S + half * rows
                abuf[half, j, :, h * HD:(h + 1) * HD] = of[r:r + rows, :].astype(jnp.bfloat16)
                tot = jnp.where(low == h, lf[r:r + rows, :], tot)
            hi = tot.astype(jnp.bfloat16).astype(jnp.float32)
            mid = (tot - hi).astype(jnp.bfloat16).astype(jnp.float32)
            rest = tot - hi - mid
            packed = jnp.where(lane < 32, hi, jnp.where(lane < 64, mid, rest))
            abuf[half, j, :, ph * HD:] = packed.astype(jnp.bfloat16)
        for p in range(1, n):
            j = lax.rem(mine + p, n)
            c = remote(
                abuf.at[half, j], arecv.at[half, mine], asend.at[half, p], ars.at[half, p],
                j // K, lax.rem(j, K),
            )
            c.start()
            acopies.append(c)
        arecv[half, mine] = abuf[half, mine]

    parts = []
    for half in range(2):
        for c in acopies[half * (n - 1):(half + 1) * (n - 1)]:
            c.wait_recv()
        fresh = fpart[0, half * rows:(half + 1) * rows, :]
        value = fpart[1, half * rows:(half + 1) * rows, :]
        lse = []
        best = fresh
        for j in range(n):
            e = arecv[half, j, :, ph * HD:].astype(jnp.float32)
            e = e + pltpu.roll(e, 96, 1) + pltpu.roll(e, 64, 1)
            lse.append(e)
            best = jnp.maximum(best, e)
        fw = jnp.exp2(fresh - best)
        total = fw
        ws = []
        for j in range(n):
            w = jnp.exp2(lse[j] - best)
            ws.append(w)
            total = total + w
        inv = 1.0 / total
        accs = []
        for h in range(ph):
            acc = (fw * inv)[:, h:h + 1] * value
            for j in range(n):
                acc = acc + (ws[j] * inv)[:, h:h + 1] * arecv[half, j, :, h * HD:(h + 1) * HD].astype(jnp.float32)
            accs.append(acc)
        parts.append(accs)
    for h in range(ph):
        both = jnp.concatenate([parts[0][h], parts[1][h]], axis=0)
        lhs[:, h * HD:(h + 1) * HD] = both.astype(jnp.bfloat16)

    pcopies, zcopies = [], []
    for s in range(T):
        w_copy(2 * s).wait()
        y = jnp.dot(lhs[...], wbuf[2 * s], preferred_element_type=jnp.float32)
        pbuf[s] = y.astype(jnp.bfloat16)
        c = remote(pbuf.at[s], precv.at[s], ps.at[s], pr.at[s], t, other)
        c.start()
        pcopies.append(c)
        w_copy(2 * s + 1).wait()
        ybuf[...] = jnp.dot(lhs[...], wbuf[2 * s + 1], preferred_element_type=jnp.float32)
        c.wait_recv()
        if s < T - 1:
            zbuf[s] = (ybuf[...] + precv[s].astype(jnp.float32)).astype(jnp.bfloat16)
            c = remote(zbuf.at[s], zrecv.at[s], zs.at[s], zr.at[s], hop(s), k)
            c.start()
            zcopies.append(c)
        else:
            ybuf[...] += precv[s].astype(jnp.float32) + res_ref[...].astype(jnp.float32)
    for c in zcopies:
        c.wait_recv()
    total = ybuf[...]
    for s in range(T - 1):
        total = total + zrecv[s].astype(jnp.float32)
    x = total.astype(jnp.bfloat16)
    full[mine] = x
    stream_ref[...] = x

    gcopies = gather_start(full, gs, gr)
    gfwd = gather_finish(full, gcopies, gfs, gfr)

    for c in qcopies + qfwd + acopies + pcopies + zcopies + gcopies + gfwd:
        c.wait_send()


def norm_kernel(part_ref, full_ref, gain_ref, stream_ref, out_ref):
    n, S, width = full_ref.shape
    stream_ref[...] = part_ref[...]
    sq = jnp.zeros((S, width), jnp.float32)
    for j in range(n):
        x = full_ref[j].astype(jnp.float32)
        sq = sq + x * x
    r = lax.rsqrt(jnp.sum(sq, axis=1, keepdims=True) / (n * width) + epsilon)
    for j in range(n):
        cols = slice(j * width, (j + 1) * width)
        gain = gain_ref[cols].astype(jnp.float32).reshape(1, width)
        out_ref[:, cols] = (full_ref[j].astype(jnp.float32) * r * gain).astype(jnp.bfloat16)


def on_device(T, K, residual, query, new_pair, kv_cache, lengths, out_weight, norm_gain):
    n = T * K
    S, width = residual.shape
    ph = query.shape[1] // HD
    span, kvh = kv_cache.shape[2:4]
    C = span * kvh
    QH = ph * n
    D = out_weight.shape[1]
    vm = pl.BlockSpec(memory_space=pltpu.VMEM)
    hbm = pl.BlockSpec(memory_space=pl.ANY)
    bf = jnp.bfloat16
    dma = pltpu.SemaphoreType.DMA
    rows = S // 2
    scratch = [
        pltpu.VMEM((2, S, kvh, HD), bf),
        pltpu.VMEM((S, width), bf),
        pltpu.VMEM((S, width), jnp.float32),
        pltpu.VMEM((2, S, C, HD), bf),
        pltpu.VMEM((n, ph * HD, width), bf),
        pltpu.VMEM((n, S, ph * HD), bf),
        pltpu.VMEM((QH * S, HD), jnp.float32),
        pltpu.VMEM((QH * S, HD), jnp.float32),
        pltpu.VMEM((QH * S, LANES), jnp.float32),
        pltpu.VMEM((QH, C), jnp.int32),
        pltpu.VMEM((2, n, rows, (ph + 1) * HD), bf),
        pltpu.VMEM((2, n, rows, (ph + 1) * HD), bf),
        pltpu.VMEM((2, S, LANES), jnp.float32),
        pltpu.VMEM((T, S, width), bf),
        pltpu.VMEM((T, S, width), bf),
        pltpu.VMEM((T, S, width), bf),
        pltpu.VMEM((T, S, width), bf),
        pltpu.VMEM((S, ph * HD), bf),
        dma((3,)),
        dma((2, S)),
        dma((n,)),
        dma((T,)), dma((T,)), dma((T,)), dma((T,)),
        dma((2, n)), dma((2, n)),
        dma((T,)), dma((T,)),
        dma((T,)), dma((T,)),
        dma((T,)), dma((T,)), dma((T,)), dma((T,)),
    ]
    part, full = pl.pallas_call(
        functools.partial(kernel, T, K, kvh),
        out_shape=(VOUT((S, width), bf), VOUT((n, S, width), bf)),
        in_specs=[pl.BlockSpec(memory_space=pltpu.SMEM)] + [hbm] * 5,
        out_specs=(vm, vm),
        scratch_shapes=scratch,
        compiler_params=pltpu.CompilerParams(
            collective_id=0, has_side_effects=True, vmem_limit_bytes=58 * 1024 * 1024
        ),
    )(lengths, query, new_pair, kv_cache.reshape(2, S, C, HD), out_weight, residual)
    return pl.pallas_call(
        norm_kernel,
        out_shape=(jax.ShapeDtypeStruct((S, width), bf), jax.ShapeDtypeStruct((S, D), bf)),
        in_specs=[vm, vm, vm],
        out_specs=(vm, vm),
        compiler_params=pltpu.CompilerParams(vmem_limit_bytes=8 * 1024 * 1024),
    )(part, full, norm_gain)


def solution(mesh):
    T, K = mesh.shape["tensor"], mesh.shape["kv"]
    seqs = ("groups", "dp")
    split = ("tensor", "kv")
    placed = (
        P(seqs, split),
        P(seqs, split),
        P(None, seqs, None, None),
        P(None, seqs, split, None, None),
        P(seqs),
        P(split, None),
        P(),
    )
    return jax.shard_map(
        functools.partial(on_device, T, K),
        mesh=mesh,
        in_specs=placed,
        out_specs=(P(seqs, split), P(seqs, None)),
        check_vma=False,
    )
```

```python
import functools
import math

import jax
import jax.numpy as jnp
from jax import lax
from jax.experimental import pallas as pl
from jax.experimental.pallas import tpu as pltpu
from jax.sharding import PartitionSpec as P

HD = 128
LANES = 128
floor_value = -1e30
epsilon = 1e-05
MESH = pl.DeviceIdType.MESH
VOUT = pltpu.VMEM


def kernel(
    T, K, kvh,
    lens_ref, q_hbm, pair_hbm, kv_hbm, w_hbm, res_hbm,
    stream_ref, full,
    pair_ref, res_ref, ybuf, kv, wbuf, qg, qf, of, lf, colid, abuf, arecv, fpart, pbuf, precv, zbuf, zrecv, lhs,
    small_sem, kv_sem, w_sem, qs, qr, qfs, qfr, asend, ars, ps, pr, zs, zr, gs, gr, gfs, gfr,
):
    t = lax.axis_index("tensor")
    k = lax.axis_index("kv")
    n = T * K
    mine = t * K + k
    other = K - 1 - k
    S, width = res_ref.shape
    ph = q_hbm.shape[1] // HD
    QH = ph * n
    group = QH // kvh
    C = kv.shape[2]
    span = C // kvh
    rows = S // 2
    hw = width // 2

    barrier = pltpu.get_barrier_semaphore()
    for p in range(1, n):
        j = lax.rem(mine + p, n)
        pl.semaphore_signal(
            barrier, inc=1, device_id={"tensor": j // K, "kv": lax.rem(j, K)}, device_id_type=MESH
        )

    small = [
        pltpu.make_async_copy(q_hbm, qg.at[mine], small_sem.at[0]),
        pltpu.make_async_copy(pair_hbm, pair_ref, small_sem.at[1]),
        pltpu.make_async_copy(res_hbm, res_ref, small_sem.at[2]),
    ]
    for c in small:
        c.start()

    def kv_copy(i, b):
        return pltpu.make_async_copy(kv_hbm.at[i, b], kv.at[i, b], kv_sem.at[i, b])

    @pl.loop(0, S)
    def _(b):
        kv_copy(0, b).start()
        kv_copy(1, b).start()

    def hop(s):
        return lax.rem(t + 1 + s, T)

    def origin(s):
        return lax.rem(t + T - 1 - s, T)

    def w_copy(s):
        dest = hop(s // 2) * K + (k if s % 2 else other)
        cols = pl.ds(pl.multiple_of(dest * width, width), width)
        return pltpu.make_async_copy(w_hbm.at[:, cols], wbuf.at[s], w_sem.at[s])

    for s in range(n):
        w_copy(s).start()

    small[0].wait()
    pl.semaphore_wait(barrier, n - 1)

    def remote(src, dst, ss, rs, tt, kk):
        return pltpu.make_async_remote_copy(
            src_ref=src, dst_ref=dst, send_sem=ss, recv_sem=rs,
            device_id={"tensor": tt, "kv": kk}, device_id_type=MESH,
        )

    def gather_start(view, ss, rs):
        out = []
        for s in range(T - 1):
            c = remote(view(mine), view(mine), ss.at[s], rs.at[s], hop(s), k)
            c.start()
            out.append(c)
        c = remote(view(mine), view(mine), ss.at[T - 1], rs.at[T - 1], t, other)
        c.start()
        out.append(c)
        return out

    def gather_finish(view, copies, fs, fr):
        fwd = []
        order = sorted(range(T - 1), key=lambda s: min(s + 1, T - 1 - s))
        for s in order:
            copies[s].wait_recv()
            j = origin(s) * K + k
            c = remote(view(j), view(j), fs.at[s], fr.at[s], t, other)
            c.start()
            fwd.append(c)
        copies[T - 1].wait_recv()
        for c in fwd:
            c.wait_recv()
        return fwd

    qcopies = gather_start(lambda j: qg.at[j], qs, qr)

    col = lax.broadcasted_iota(jnp.int32, (QH, C), 1)
    head = lax.broadcasted_iota(jnp.int32, (QH, C), 0)
    colid[...] = jnp.where(lax.rem(col, kvh) == head // group, col, jnp.int32(2**30))
    scale2 = math.log2(math.e) / math.sqrt(HD)
    my_group = (mine * ph) // group
    fkey = jnp.zeros((S, HD), jnp.float32)
    fval = jnp.zeros((S, HD), jnp.float32)
    small[1].wait()
    small[2].wait()
    for g in range(kvh):
        fkey = jnp.where(my_group == g, pair_ref[0, :, g, :].astype(jnp.float32), fkey)
        fval = jnp.where(my_group == g, pair_ref[1, :, g, :].astype(jnp.float32), fval)
    lane = lax.broadcasted_iota(jnp.int32, (S, LANES), 1)
    fresh = jnp.zeros((S, LANES), jnp.float32)
    for h in range(ph):
        prod = qg[mine, :, h * HD:(h + 1) * HD].astype(jnp.float32) * fkey
        fresh = jnp.where(lane == h, jnp.sum(prod, axis=1, keepdims=True) * scale2, fresh)
    fpart[0] = fresh
    fpart[1] = fval

    qfwd = gather_finish(lambda j: qg.at[j], qcopies, qfs, qfr)
    for j in range(n):
        for h in range(ph):
            r = (j * ph + h) * S
            qf[r:r + S, :] = qg[j, :, h * HD:(h + 1) * HD].astype(jnp.float32)

    start = mine * span

    def attend(b, _):
        kv_copy(0, b).wait()
        kv_copy(1, b).wait()
        qb = qf[pl.ds(b, QH, stride=S), :].astype(jnp.bfloat16)
        s = lax.dot_general(qb, kv[0, b], (((1,), (1,)), ((), ())), preferred_element_type=jnp.float32)
        lim = (lens_ref[b] - start) * kvh
        s = jnp.where(colid[...] < lim, s * scale2, floor_value)
        m = jnp.maximum(jnp.max(s, axis=1, keepdims=True), -1e29)
        p = jnp.exp2(s - m)
        l = jnp.maximum(jnp.sum(p, axis=1, keepdims=True), 1.0)
        o = jnp.dot(p.astype(jnp.bfloat16), kv[1, b], preferred_element_type=jnp.float32)
        of[pl.ds(b, QH, stride=S), :] = o / l
        lf[pl.ds(b, QH, stride=S), :] = jnp.broadcast_to(m + jnp.log2(l), (QH, LANES))
        return 0

    lane = lax.broadcasted_iota(jnp.int32, (rows, LANES), 1)
    low = lax.rem(lane, 32)
    acopies = []
    for half in range(2):
        lax.fori_loop(half * rows, (half + 1) * rows, attend, 0, unroll=4)
        for j in range(n):
            tot = jnp.zeros((rows, LANES), jnp.float32)
            for h in range(ph):
                r = (j * ph + h) * S + half * rows
                abuf[half, j, :, h * HD:(h + 1) * HD] = of[r:r + rows, :].astype(jnp.bfloat16)
                tot = jnp.where(low == h, lf[r:r + rows, :], tot)
            hi = tot.astype(jnp.bfloat16).astype(jnp.float32)
            mid = (tot - hi).astype(jnp.bfloat16).astype(jnp.float32)
            rest = tot - hi - mid
            packed = jnp.where(lane < 32, hi, jnp.where(lane < 64, mid, rest))
            abuf[half, j, :, ph * HD:] = packed.astype(jnp.bfloat16)
        for p in range(1, n):
            j = lax.rem(mine + p, n)
            c = remote(
                abuf.at[half, j], arecv.at[half, mine], asend.at[half, p], ars.at[half, p],
                j // K, lax.rem(j, K),
            )
            c.start()
            acopies.append(c)
        arecv[half, mine] = abuf[half, mine]

    parts = []
    for half in range(2):
        for c in acopies[half * (n - 1):(half + 1) * (n - 1)]:
            c.wait_recv()
        fresh = fpart[0, half * rows:(half + 1) * rows, :]
        value = fpart[1, half * rows:(half + 1) * rows, :]
        lse = []
        best = fresh
        for j in range(n):
            e = arecv[half, j, :, ph * HD:].astype(jnp.float32)
            e = e + pltpu.roll(e, 96, 1) + pltpu.roll(e, 64, 1)
            lse.append(e)
            best = jnp.maximum(best, e)
        fw = jnp.exp2(fresh - best)
        total = fw
        ws = []
        for j in range(n):
            w = jnp.exp2(lse[j] - best)
            ws.append(w)
            total = total + w
        inv = 1.0 / total
        accs = []
        for h in range(ph):
            acc = (fw * inv)[:, h:h + 1] * value
            for j in range(n):
                acc = acc + (ws[j] * inv)[:, h:h + 1] * arecv[half, j, :, h * HD:(h + 1) * HD].astype(jnp.float32)
            accs.append(acc)
        parts.append(accs)
    for h in range(ph):
        both = jnp.concatenate([parts[0][h], parts[1][h]], axis=0)
        lhs[:, h * HD:(h + 1) * HD] = both.astype(jnp.bfloat16)

    pcopies, zcopies = [], []

    def project(half):
        cols = slice(half * hw, (half + 1) * hw)
        for s in range(T):
            if half == 0:
                w_copy(2 * s).wait()
            y = jnp.dot(lhs[...], wbuf[2 * s, :, cols], preferred_element_type=jnp.float32)
            pbuf[half, s] = y.astype(jnp.bfloat16)
            c = remote(pbuf.at[half, s], precv.at[half, s], ps.at[half, s], pr.at[half, s], t, other)
            c.start()
            pcopies.append(c)
            if half == 0:
                w_copy(2 * s + 1).wait()
            ybuf[half] = jnp.dot(lhs[...], wbuf[2 * s + 1, :, cols], preferred_element_type=jnp.float32)
            c.wait_recv()
            y = ybuf[half] + precv[half, s].astype(jnp.float32)
            if s < T - 1:
                zbuf[half, s] = y.astype(jnp.bfloat16)
                c = remote(zbuf.at[half, s], zrecv.at[half, s], zs.at[half, s], zr.at[half, s], hop(s), k)
                c.start()
                zcopies.append(c)
            else:
                ybuf[half] = y + res_ref[:, cols].astype(jnp.float32)

    gcopies, gfwd = [], []

    def view(half):
        return lambda j: full.at[j, :, pl.ds(half * hw, hw)]

    def settle(half):
        cols = slice(half * hw, (half + 1) * hw)
        for c in zcopies[half * (T - 1):(half + 1) * (T - 1)]:
            c.wait_recv()
        total = ybuf[half]
        for s in range(T - 1):
            total = total + zrecv[half, s].astype(jnp.float32)
        x = total.astype(jnp.bfloat16)
        full[mine, :, cols] = x
        stream_ref[:, cols] = x
        gcopies.extend(gather_start(view(half), gs.at[half], gr.at[half]))

    project(0)
    project(1)
    settle(0)
    settle(1)
    for half in range(2):
        mine_copies = gcopies[half * T:(half + 1) * T]
        gfwd.extend(gather_finish(view(half), mine_copies, gfs.at[half], gfr.at[half]))

    for c in qcopies + qfwd + acopies + pcopies + zcopies + gcopies + gfwd:
        c.wait_send()


def norm_kernel(part_ref, full_ref, gain_ref, stream_ref, out_ref):
    n, S, width = full_ref.shape
    stream_ref[...] = part_ref[...]
    sq = jnp.zeros((S, width), jnp.float32)
    for j in range(n):
        x = full_ref[j].astype(jnp.float32)
        sq = sq + x * x
    r = lax.rsqrt(jnp.sum(sq, axis=1, keepdims=True) / (n * width) + epsilon)
    for j in range(n):
        cols = slice(j * width, (j + 1) * width)
        gain = gain_ref[cols].astype(jnp.float32).reshape(1, width)
        out_ref[:, cols] = (full_ref[j].astype(jnp.float32) * r * gain).astype(jnp.bfloat16)


def on_device(T, K, residual, query, new_pair, kv_cache, lengths, out_weight, norm_gain):
    n = T * K
    S, width = residual.shape
    ph = query.shape[1] // HD
    span, kvh = kv_cache.shape[2:4]
    C = span * kvh
    QH = ph * n
    D = out_weight.shape[1]
    vm = pl.BlockSpec(memory_space=pltpu.VMEM)
    hbm = pl.BlockSpec(memory_space=pl.ANY)
    bf = jnp.bfloat16
    dma = pltpu.SemaphoreType.DMA
    rows = S // 2
    scratch = [
        pltpu.VMEM((2, S, kvh, HD), bf),
        pltpu.VMEM((S, width), bf),
        pltpu.VMEM((2, S, width // 2), jnp.float32),
        pltpu.VMEM((2, S, C, HD), bf),
        pltpu.VMEM((n, ph * HD, width), bf),
        pltpu.VMEM((n, S, ph * HD), bf),
        pltpu.VMEM((QH * S, HD), jnp.float32),
        pltpu.VMEM((QH * S, HD), jnp.float32),
        pltpu.VMEM((QH * S, LANES), jnp.float32),
        pltpu.VMEM((QH, C), jnp.int32),
        pltpu.VMEM((2, n, rows, (ph + 1) * HD), bf),
        pltpu.VMEM((2, n, rows, (ph + 1) * HD), bf),
        pltpu.VMEM((2, S, LANES), jnp.float32),
        pltpu.VMEM((2, T, S, width // 2), bf),
        pltpu.VMEM((2, T, S, width // 2), bf),
        pltpu.VMEM((2, T, S, width // 2), bf),
        pltpu.VMEM((2, T, S, width // 2), bf),
        pltpu.VMEM((S, ph * HD), bf),
        dma((3,)),
        dma((2, S)),
        dma((n,)),
        dma((T,)), dma((T,)), dma((T,)), dma((T,)),
        dma((2, n)), dma((2, n)),
        dma((2, T)), dma((2, T)),
        dma((2, T)), dma((2, T)),
        dma((2, T)), dma((2, T)), dma((2, T)), dma((2, T)),
    ]
    part, full = pl.pallas_call(
        functools.partial(kernel, T, K, kvh),
        out_shape=(VOUT((S, width), bf), VOUT((n, S, width), bf)),
        in_specs=[pl.BlockSpec(memory_space=pltpu.SMEM)] + [hbm] * 5,
        out_specs=(vm, vm),
        scratch_shapes=scratch,
        compiler_params=pltpu.CompilerParams(
            collective_id=0, has_side_effects=True, vmem_limit_bytes=58 * 1024 * 1024
        ),
    )(lengths, query, new_pair, kv_cache.reshape(2, S, C, HD), out_weight, residual)
    return pl.pallas_call(
        norm_kernel,
        out_shape=(jax.ShapeDtypeStruct((S, width), bf), jax.ShapeDtypeStruct((S, D), bf)),
        in_specs=[vm, vm, vm],
        out_specs=(vm, vm),
        compiler_params=pltpu.CompilerParams(vmem_limit_bytes=8 * 1024 * 1024),
    )(part, full, norm_gain)


def solution(mesh):
    T, K = mesh.shape["tensor"], mesh.shape["kv"]
    seqs = ("groups", "dp")
    split = ("tensor", "kv")
    placed = (
        P(seqs, split),
        P(seqs, split),
        P(None, seqs, None, None),
        P(None, seqs, split, None, None),
        P(seqs),
        P(split, None),
        P(),
    )
    return jax.shard_map(
        functools.partial(on_device, T, K),
        mesh=mesh,
        in_specs=placed,
        out_specs=(P(seqs, split), P(seqs, None)),
        check_vma=False,
    )
```
